128 devices in a mesh: grp: 64 (over x, z, y), rep: 2 (over core).
Axes of the slice: x: 4, y: 4, z: 4, core: 2. Of those that a mesh axis runs over, the one named last changes fastest.
Arguments:
- states: float32 [16384, 1024], P(('grp', 'rep')), may hold values from 0 to 1
- coupling: bfloat16 [1024, 2048], replicated, may hold values from -0.1875 to 0.1875
- vis_bias: float32 [1024], replicated, may hold values from -6 to 6
- hid_bias: float32 [2048], replicated, may hold values from -6 to 6
- noise: bfloat16 [4, 16384, 2048], P(None, ('grp', 'rep')), may hold values from -6 to 6
- tickets: int32 [16384], P(('grp', 'rep')), may hold values from 1 to 4
- offset: int32 [1], replicated, may hold values from 0 to 16383
Outputs:
- visible: float32 [16384, 1024], P(('grp', 'rep'))
- weights: float32 [16384], P(('grp', 'rep'))
- log_ratio: float32 [], replicated
The draws below stay inside these ranges and needn't reach their ends.
All inputs are finite; a program needn't handle non-finite values.
Results may differ from the reference program's by a relative error of at most 0.0047.
Values may be sent and summed in bfloat16 or wider, within the bound.
A program may use at most 64 MiB of HBM per device.

```python
import jax
import jax.numpy as jnp

V = 1024
H = 2048
CH_DEV = 128
SWEEPS = 4
CHAINS = 16384
N_GRP = 64
N_REP = 2


def draw_tickets(key, part):
    key_base = jax.random.fold_in(key, 11)
    key_heavy = jax.random.fold_in(key, 12)
    key_upper = jax.random.fold_in(key, 13)
    key_hot = jax.random.fold_in(key, 14)
    groups = CHAINS // CH_DEV
    lower_draw = jax.random.randint(key_base, (groups, CH_DEV), 1, 3)
    heavy_flag = jax.random.randint(key_heavy, (groups, 1), 0, 8) == 0
    upper_draw = jax.random.randint(key_upper, (groups, CH_DEV), 2, 5)
    hot_device = jax.random.randint(key_hot, (), 0, groups)
    picked = jnp.where(heavy_flag, upper_draw, lower_draw)
    picked = jnp.where(jnp.arange(groups)[:, None] == hot_device, 4, picked)
    return picked.reshape(-1).astype(jnp.int32)


def shard_levels(own_key, shape, shards, low, top_value):
    level = 1.0
    for position, parts in shards:
        steps = jax.random.uniform(jax.random.fold_in(jax.random.fold_in(own_key, 6), position), (parts,), jnp.float32, low / len(shards), top_value / len(shards))
        level = level * jnp.repeat(jnp.exp(steps), shape[position] // parts).reshape((-1,) + (1,) * (len(shape) - 1 - position))
    return level


def scatter_about(key, shape, width, limit, shards=(), kind=jnp.bfloat16):
    result = jax.random.normal(key, shape, jnp.float32) * width
    if len(shards) > 0:
        result = shard_levels(key, shape, shards, -0.22, 0.18) * result
    return jnp.clip(result, min=-limit, max=limit).astype(kind)


def setup_inputs(seed: int = 0) -> dict:
    key_list = jax.random.split(jax.random.key(seed), 8)
    return {
        "states": jnp.clip(1.0 * jax.random.uniform(key_list[0], (CHAINS, V), jnp.float32) ** shard_levels(key_list[0], (CHAINS, V), ((0, 128),), -0.2, 0.2), 0.0, 1.0),
        "coupling": scatter_about(key_list[1], (V, H), V ** -0.5, 0.1875),
        "vis_bias": scatter_about(key_list[2], (V,), 1.0, 6.0, (), jnp.float32),
        "hid_bias": scatter_about(key_list[3], (H,), 1.0, 6.0, (), jnp.float32),
        "noise": scatter_about(key_list[4], (SWEEPS, CHAINS, H), 1.0, 6.0, ((1, 128),)),
        "tickets": draw_tickets(jax.random.fold_in(key_list[7], 71), 0),
        "offset": jax.random.randint(key_list[6], (1,), 0, CHAINS).astype(jnp.int32),
    }


def reference(states, coupling, vis_bias, hid_bias, noise, tickets, offset):
    chains = tickets.shape[0]
    devices = N_GRP * N_REP
    beta_step = 204.8 / H
    cumulative = jnp.cumsum(tickets).astype(jnp.int32)
    grand_total = cumulative[-1]
    jitter = offset[0].astype(jnp.int32)
    slots = jnp.arange(chains, dtype=jnp.int32)
    points = (slots * (grand_total // chains) + (slots * (grand_total % chains) + jitter) // chains).astype(jnp.int32)
    parent = jnp.searchsorted(cumulative, points, side="right").astype(jnp.int32)
    row_order = (jnp.arange(devices, dtype=jnp.int32)[:, None] + devices * jnp.arange(CH_DEV, dtype=jnp.int32)[None, :]).reshape(-1)
    source = parent[row_order]
    visible_b = states[source].astype(jnp.bfloat16)
    visible = visible_b.astype(jnp.float32)
    for sweep_idx in range(SWEEPS):
        pre_hidden = jnp.dot(visible_b, coupling, preferred_element_type=jnp.float32)
        hidden = jax.nn.sigmoid(pre_hidden + hid_bias + noise[sweep_idx].astype(jnp.float32)).astype(jnp.bfloat16)
        pre_visible = jnp.dot(hidden, coupling.T, preferred_element_type=jnp.float32)
        visible = 0.5 * visible + 0.5 * jax.nn.sigmoid(pre_visible + vis_bias)
        visible_b = visible.astype(jnp.bfloat16)
    activity = jnp.dot(visible_b, coupling, preferred_element_type=jnp.float32) + hid_bias
    log_weight = beta_step * (jnp.sum(visible * vis_bias, axis=-1) + jnp.sum(jax.nn.softplus(activity), axis=-1))
    highest = jnp.max(log_weight)
    shifted = jnp.exp(log_weight - highest)
    mass_sum = jnp.sum(shifted)
    weights = shifted * (chains / mass_sum)
    log_ratio = highest + jnp.log(mass_sum) - jnp.log(jnp.float32(chains))
    return visible, weights, log_ratio
```

```python
import jax
import jax.numpy as jnp
from jax import lax
from jax.experimental import pallas as pl
from jax.experimental.pallas import tpu as pltpu
from jax.sharding import PartitionSpec as P

MESH = pl.DeviceIdType.MESH
SWEEPS = 4
ROWS = 128
GROUP = 8
GROUPS = 16
CAP = 32
SHIFT = 14
CHAINS = 1 << SHIFT


def where_is(t):
    return (t // 2, lax.rem(t, 2))


def remote(src, dst, send, recv, t):
    return pltpu.make_async_remote_copy(
        src_ref=src,
        dst_ref=dst,
        send_sem=send,
        recv_sem=recv,
        device_id=where_is(t),
        device_id_type=MESH,
    )


def wait_bytes(ref, sem):
    pltpu.make_async_copy(ref, ref, sem).wait()


def logistic(x):
    return 0.5 * jnp.tanh(0.5 * x) + 0.5


def step_kernel(
    states_ref,
    coupling_ref,
    vis_bias_ref,
    hid_bias_ref,
    noise_ref,
    tickets_ref,
    offset_ref,
    visible_ref,
    weights_ref,
    ratio_ref,
    own_tickets,
    group_tickets,
    all_tickets,
    vis,
    pool,
    onehot,
    outbox,
    inbox,
    cpl,
    cpl_t,
    nz,
    hb,
    vb,
    hid,
    visb,
    own_stat,
    group_stats,
    all_stats,
    load_sems,
    tick_sems,
    ring_send,
    ring_recv,
    pair_send,
    pair_recv,
    rows_send,
    rows_recv,
    stat_sems,
    out_sem,
):
    me = lax.axis_index("grp") * 2 + lax.axis_index("rep")
    core = lax.rem(me, 2)
    seat = lax.rem(me, GROUP)
    line = lax.rem(me // 2, 4)
    group = me // GROUP
    gx, gz = group // 4, lax.rem(group, 4)
    base = me - seat
    sibling = me + 1 - 2 * core
    up = base + 2 * lax.rem(line + 1, 4) + core
    down = base + 2 * lax.rem(line + 3, 4) + core
    mates = [base + lax.rem(seat + i, GROUP) for i in range(1, GROUP)]

    def plane(i):
        return 4 * lax.rem(gx + i // 4, 4) + lax.rem(gz + i % 4, 4)

    rows = [GROUP * plane(i) + seat for i in range(1, GROUPS)]

    barrier = pltpu.get_barrier_semaphore()
    for t in mates + rows:
        pl.semaphore_signal(barrier, inc=1, device_id=where_is(t), device_id_type=MESH)

    loads = [
        pltpu.make_async_copy(src, dst, load_sems.at[i])
        for i, (src, dst) in enumerate(
            (
                (tickets_ref, own_tickets),
                (states_ref, vis),
                (coupling_ref, cpl),
                (noise_ref, nz),
                (hid_bias_ref, hb),
                (vis_bias_ref, vb),
            )
        )
    ]
    for copy in loads:
        copy.start()
    loads[0].wait()
    group_tickets[pl.ds(seat, 1), :] = own_tickets[...]
    loads[1].wait()

    def block(owner, half=None):
        if half is None:
            return pool.at[pl.ds(pl.multiple_of(owner * ROWS, ROWS), ROWS)]
        start = pl.multiple_of(owner * ROWS + half * (ROWS // 2), ROWS // 2)
        return pool.at[pl.ds(start, ROWS // 2)]

    pool[pl.ds(pl.multiple_of(seat * ROWS, ROWS), ROWS), :] = vis[...].astype(jnp.bfloat16)
    pl.semaphore_wait(barrier, GROUP - 1 + GROUPS - 1)

    for t in mates:
        remote(
            own_tickets, group_tickets.at[pl.ds(seat, 1)], tick_sems.at[0], tick_sems.at[1], t
        ).start()
    sends = []

    def ring(owner, half, to_up, slot):
        copy = remote(
            block(owner, half),
            block(owner, half),
            ring_send.at[slot],
            ring_recv.at[slot],
            up if to_up else down,
        )
        copy.start()
        sends.append(copy)

    def hand(owner, half, slot):
        copy = remote(
            block(owner, half), block(owner, half), pair_send.at[slot], pair_recv, sibling
        )
        copy.start()
        sends.append(copy)

    prev = lax.rem(seat + 6, GROUP)
    after = lax.rem(seat + 2, GROUP)
    across = lax.rem(seat + 4, GROUP)
    ring(seat, 0, True, 0)
    ring(seat, 1, False, 1)
    ring(seat, 1, True, 2)
    ring(seat, 0, False, 3)
    hand(seat, None, 0)

    wait_bytes(group_tickets.at[pl.ds(0, GROUP - 1)], tick_sems.at[1])
    my_rows = pl.ds(pl.multiple_of(base, GROUP), GROUP)
    all_tickets[my_rows, :] = group_tickets[...]
    for t in rows:
        remote(
            group_tickets, all_tickets.at[my_rows], tick_sems.at[2], tick_sems.at[3], t
        ).start()

    wait_bytes(block(prev, 0), ring_recv.at[0])
    ring(prev, 0, True, 4)
    hand(prev, 0, 1)
    wait_bytes(block(after, 1), ring_recv.at[1])
    ring(after, 1, False, 5)
    hand(after, 1, 2)

    wait_bytes(all_tickets.at[pl.ds(0, (GROUPS - 1) * GROUP)], tick_sems.at[3])
    everything = all_tickets[...].astype(jnp.float32)
    totals = jnp.sum(everything, axis=1, keepdims=True)
    grand = jnp.sum(totals, axis=0, keepdims=True).astype(jnp.int32)
    z_high, z_low = grand >> SHIFT, grand & (CHAINS - 1)
    jitter = offset_ref[0]

    def point(k):
        return k * z_high + ((k * z_low + jitter) >> SHIFT)

    def count(mask, axis):
        return jnp.sum(jnp.where(mask, 1.0, 0.0), axis=axis, keepdims=True).astype(jnp.int32)

    device = lax.broadcasted_iota(jnp.int32, (ROWS, 1), 0)
    before = jnp.sum(jnp.where(device < base, totals, 0.0), axis=0, keepdims=True)
    group_first = before.astype(jnp.int32)

    slot_row = lax.broadcasted_iota(jnp.int32, (GROUPS * CAP, 1), 0)
    turn = slot_row // CAP
    target = 4 * ((gx + turn // 4) & 3) + ((gz + turn) & 3)
    heir = GROUP * target + seat
    lane = lax.broadcasted_iota(jnp.int32, (1, ROWS), 1)
    first = count(point(lane * ROWS + heir) < group_first, 1)
    place = first + (slot_row & (CAP - 1))
    level = jnp.where(place < ROWS, point(place * ROWS + heir), jnp.int32(1 << 30))
    lower = lax.broadcasted_iota(jnp.int32, (ROWS, ROWS), 0) <= lax.broadcasted_iota(
        jnp.int32, (ROWS, ROWS), 1
    )
    mine = group_tickets[...]
    inner = jnp.dot(
        mine.astype(jnp.float32).astype(jnp.bfloat16),
        jnp.where(lower, 1.0, 0.0).astype(jnp.bfloat16),
        preferred_element_type=jnp.float32,
    )
    opened = before
    for d in range(GROUP):
        high = (opened + inner[d : d + 1, :]).astype(jnp.int32)
        low = high - mine[d : d + 1, :]
        onehot[:, d * ROWS : (d + 1) * ROWS] = jnp.where(
            (level >= low) & (level < high), 1.0, 0.0
        ).astype(jnp.bfloat16)
        opened = opened + inner[d : d + 1, ROWS - 1 : ROWS]

    wait_bytes(block(prev, 1), ring_recv.at[2])
    hand(prev, 1, 3)
    wait_bytes(block(after, 0), ring_recv.at[3])
    hand(after, 0, 4)
    wait_bytes(block(across, 0), ring_recv.at[4])
    hand(across, 0, 5)
    wait_bytes(block(across, 1), ring_recv.at[5])
    hand(across, 1, 6)
    wait_bytes(pool.at[pl.ds(0, 4 * ROWS)], pair_recv)

    home = pl.ds(pl.multiple_of(group * CAP, CAP), CAP)
    for part in range(4):
        chunk = slice(part * 4 * CAP, (part + 1) * 4 * CAP)
        outbox[chunk, :] = jnp.dot(
            onehot[chunk, :], pool[...], preferred_element_type=jnp.float32
        ).astype(jnp.bfloat16)
        for i in range(4 * part, 4 * part + 4):
            if i == 0:
                inbox[home, :] = outbox[0:CAP, :]
            else:
                remote(
                    outbox.at[pl.ds(i * CAP, CAP)], inbox.at[home], rows_send, rows_recv, rows[i - 1]
                ).start()

    loads[2].wait()

    def turn_over(i, carry):
        cols = pl.ds(pl.multiple_of(i * 256, 256), 256)
        for j in range(0, 1024, 256):
            cpl_t[cols, j : j + 256] = cpl[j : j + 256, cols].T
        return carry

    lax.fori_loop(0, 8, turn_over, 0)

    mark = lax.broadcasted_iota(jnp.int32, (1, GROUPS * CAP), 1)
    origin = mark // CAP
    opens = jnp.sum(
        jnp.where(device < GROUP * origin, totals, 0.0), axis=0, keepdims=True
    ).astype(jnp.int32)
    closes = jnp.sum(
        jnp.where(device < GROUP * origin + GROUP, totals, 0.0), axis=0, keepdims=True
    ).astype(jnp.int32)
    needs = point(device * ROWS + me)
    skipped = count(needs < opens, 0)
    chosen = (device - skipped == (mark & (CAP - 1))) & (needs >= opens) & (needs < closes)
    selector = jnp.where(chosen, 1.0, 0.0).astype(jnp.bfloat16)

    for copy in loads[3:]:
        copy.wait()
    wait_bytes(inbox.at[pl.ds(0, (GROUPS - 1) * CAP)], rows_recv)
    start = jnp.dot(selector, inbox[...], preferred_element_type=jnp.float32)
    vis[...] = start
    visb[...] = start.astype(jnp.bfloat16)

    def sweep(s, carry):
        for n in range(0, 2048, 256):
            cols = slice(n, n + 256)
            pre = jnp.dot(visb[...], cpl[:, cols], preferred_element_type=jnp.float32)
            field = pre + hb[:, cols] + nz[s, :, cols].astype(jnp.float32)
            hid[:, cols] = logistic(field).astype(jnp.bfloat16)
        for n in range(0, 1024, 256):
            cols = slice(n, n + 256)
            pre = jnp.dot(hid[...], cpl_t[:, cols], preferred_element_type=jnp.float32)
            new = 0.5 * vis[:, cols] + 0.5 * logistic(pre + vb[:, cols])
            vis[:, cols] = new
            visb[:, cols] = new.astype(jnp.bfloat16)
        return carry

    lax.fori_loop(0, SWEEPS, sweep, 0)
    result = pltpu.make_async_copy(vis, visible_ref, out_sem)
    result.start()

    energy = jnp.sum(vis[...] * vb[...], axis=1, keepdims=True)
    for n in range(0, 2048, 256):
        cols = slice(n, n + 256)
        act = jnp.dot(visb[...], cpl[:, cols], preferred_element_type=jnp.float32) + hb[:, cols]
        soft = jnp.maximum(act, 0.0) + jnp.log(1.0 + jnp.exp(-jnp.abs(act)))
        energy = energy + jnp.sum(soft, axis=1, keepdims=True)
    beta_step = 204.8 / 2048
    log_weight = beta_step * energy
    diagonal = device == lane
    flat = jnp.sum(jnp.where(diagonal, log_weight, 0.0), axis=0, keepdims=True)

    def packed(top, total):
        return jnp.where(lane < ROWS // 2, top, total)

    def merged(ref):
        both = ref[...]
        sums = pltpu.roll(both, ROWS // 2, 1)
        head = lax.broadcasted_iota(jnp.int32, both.shape, 1) < ROWS // 2
        top = jnp.max(jnp.where(head, both, -jnp.inf), axis=(0, 1), keepdims=True)
        one = lax.broadcasted_iota(jnp.int32, both.shape, 1) == 0
        scaled = jnp.where(one, sums * jnp.exp(jnp.where(one, both, top) - top), 0.0)
        return top, jnp.sum(scaled, axis=(0, 1), keepdims=True)

    top = jnp.max(flat, axis=1, keepdims=True)
    total = jnp.sum(jnp.exp(flat - top), axis=1, keepdims=True)
    own_stat[0:1, :] = packed(top, total)
    group_stats[pl.ds(seat, 1), :] = packed(top, total)
    for t in mates:
        remote(
            own_stat.at[pl.ds(0, 1)],
            group_stats.at[pl.ds(seat, 1)],
            stat_sems.at[0],
            stat_sems.at[1],
            t,
        ).start()
    wait_bytes(group_stats.at[pl.ds(0, GROUP - 1)], stat_sems.at[1])
    top, total = merged(group_stats)
    own_stat[8:9, :] = packed(top, total)
    all_stats[pl.ds(group, 1), :] = packed(top, total)
    for t in rows:
        remote(
            own_stat.at[pl.ds(8, 1)],
            all_stats.at[pl.ds(group, 1)],
            stat_sems.at[2],
            stat_sems.at[3],
            t,
        ).start()

    for copy in sends:
        copy.wait_send()
    wait_bytes(group_tickets.at[pl.ds(0, GROUP - 1)], tick_sems.at[0])
    wait_bytes(all_tickets.at[pl.ds(0, (GROUPS - 1) * GROUP)], tick_sems.at[2])
    wait_bytes(outbox.at[pl.ds(CAP, (GROUPS - 1) * CAP)], rows_send)
    wait_bytes(group_stats.at[pl.ds(0, GROUP - 1)], stat_sems.at[0])

    wait_bytes(all_stats.at[pl.ds(0, GROUPS - 1)], stat_sems.at[3])
    top, total = merged(all_stats)
    weights_ref[...] = jnp.exp(flat - top) * (CHAINS / total)
    ratio_ref[...] = top + jnp.log(total) - jnp.log(jnp.full((1, 1), CHAINS, jnp.float32))
    wait_bytes(all_stats.at[pl.ds(0, GROUPS - 1)], stat_sems.at[2])
    result.wait()


def per_device(states, coupling, vis_bias, hid_bias, noise, tickets, offset):
    f32, b16, i32 = jnp.float32, jnp.bfloat16, jnp.int32
    anywhere = pl.BlockSpec(memory_space=pl.ANY)
    dma = pltpu.SemaphoreType.DMA
    visible, weights, ratio = pl.pallas_call(
        step_kernel,
        out_shape=(
            jax.ShapeDtypeStruct((ROWS, 1024), f32),
            jax.ShapeDtypeStruct((1, ROWS), f32),
            jax.ShapeDtypeStruct((1, 1), f32),
        ),
        in_specs=[anywhere] * 6 + [pl.BlockSpec(memory_space=pltpu.SMEM)],
        out_specs=(
            anywhere,
            pl.BlockSpec(memory_space=pltpu.VMEM),
            pl.BlockSpec(memory_space=pltpu.VMEM),
        ),
        scratch_shapes=[
            pltpu.VMEM((1, ROWS), i32),
            pltpu.VMEM((GROUP, ROWS), i32),
            pltpu.VMEM((ROWS, ROWS), i32),
            pltpu.VMEM((ROWS, 1024), f32),
            pltpu.VMEM((GROUP * ROWS, 1024), b16),
            pltpu.VMEM((GROUPS * CAP, GROUP * ROWS), b16),
            pltpu.VMEM((GROUPS * CAP, 1024), b16),
            pltpu.VMEM((GROUPS * CAP, 1024), b16),
            pltpu.VMEM((1024, 2048), b16),
            pltpu.VMEM((2048, 1024), b16),
            pltpu.VMEM((SWEEPS, ROWS, 2048), b16),
            pltpu.VMEM((1, 2048), f32),
            pltpu.VMEM((1, 1024), f32),
            pltpu.VMEM((ROWS, 2048), b16),
            pltpu.VMEM((ROWS, 1024), b16),
            pltpu.VMEM((16, ROWS), f32),
            pltpu.VMEM((GROUP, ROWS), f32),
            pltpu.VMEM((GROUPS, ROWS), f32),
            dma((6,)),
            dma((4,)),
            dma((6,)),
            dma((6,)),
            dma((7,)),
            dma(()),
            dma(()),
            dma(()),
            dma((4,)),
            dma(()),
        ],
        compiler_params=pltpu.CompilerParams(collective_id=1, has_side_effects=True),
    )(
        states,
        coupling,
        vis_bias.reshape(1, 1024),
        hid_bias.reshape(1, 2048),
        noise,
        tickets.reshape(1, ROWS),
        offset,
    )
    return visible, weights.reshape(ROWS), ratio.reshape(())


def solution(mesh):
    both = ("grp", "rep")
    return jax.shard_map(
        per_device,
        mesh=mesh,
        in_specs=(P(both, None), P(), P(), P(), P(None, both, None), P(both), P()),
        out_specs=(P(both, None), P(both), P()),
        check_vma=False,
    )
```

```python
import functools

import jax
import jax.numpy as jnp
from jax import lax
from jax.experimental import pallas as pl
from jax.experimental.pallas import tpu as pltpu
from jax.sharding import PartitionSpec as P

MESH = pl.DeviceIdType.MESH
SWEEPS = 4
ROWS = 128
GROUP = 4
GROUPS = 32
NARROW, WIDE = 8, 16
SHIFT = 14
CHAINS = 1 << SHIFT


def where_is(t):
    return (t // 2, lax.rem(t, 2))


def remote(src, dst, send, recv, t):
    return pltpu.make_async_remote_copy(
        src_ref=src,
        dst_ref=dst,
        send_sem=send,
        recv_sem=recv,
        device_id=where_is(t),
        device_id_type=MESH,
    )


def wait_bytes(ref, sem):
    pltpu.make_async_copy(ref, ref, sem).wait()


def logistic(x):
    return 0.5 * jnp.tanh(0.5 * x) + 0.5


def step_kernel(
    cap,
    states_ref,
    coupling_ref,
    vis_bias_ref,
    hid_bias_ref,
    noise_ref,
    tickets_ref,
    offset_hbm,
    visible_ref,
    weights_ref,
    ratio_ref,
    spill_ref,
    offset_ref,
    own_tickets,
    group_tickets,
    all_tickets,
    vis,
    pool,
    onehot,
    outbox,
    inbox,
    cpl,
    cpl_t,
    nz,
    hb,
    vb,
    hid,
    visb,
    own_stat,
    group_stats,
    all_stats,
    load_sems,
    tick_sems,
    ring_send,
    ring_recv,
    pair_send,
    pair_recv,
    rows_send,
    rows_recv,
    stat_sems,
    out_sem,
):
    me = lax.axis_index("grp") * 2 + lax.axis_index("rep")
    core = lax.rem(me, 2)
    seat = lax.rem(me, GROUP)
    line = lax.rem(me // 2, 4)
    group = me // GROUP
    gx, gz = me // 32, lax.rem(me // 8, 4)
    base = me - seat
    sibling = me + 1 - 2 * core
    partner = base + lax.rem(seat + 2, GROUP)
    mates = [base + lax.rem(seat + i, GROUP) for i in range(1, GROUP)]

    def away(i):
        x = lax.rem(gx + i // 8, 4)
        z = lax.rem(gz + i // 2 % 4, 4)
        return 8 * (4 * x + z) + 2 * (line + i % 2 * (3 - 2 * line)) + core

    def hops(i):
        return (0, 1, 2, 1)[i // 8] + (0, 1, 2, 1)[i // 2 % 4] + i % 2

    order = sorted(range(1, GROUPS), key=hops, reverse=True)
    rows = [away(i) for i in order]

    barrier = pltpu.get_barrier_semaphore()
    for t in mates + rows:
        pl.semaphore_signal(barrier, inc=1, device_id=where_is(t), device_id_type=MESH)

    loads = [
        pltpu.make_async_copy(src, dst, load_sems.at[i])
        for i, (src, dst) in enumerate(
            (
                (tickets_ref, own_tickets),
                (states_ref, vis),
                (coupling_ref, cpl),
                (noise_ref, nz),
                (hid_bias_ref, hb),
                (vis_bias_ref, vb),
                (offset_hbm, offset_ref),
            )
        )
    ]
    for copy in loads:
        copy.start()
    loads[0].wait()
    group_tickets[pl.ds(seat, 1), :] = own_tickets[...]
    loads[1].wait()

    def block(owner, half=None):
        if half is None:
            return pool.at[pl.ds(pl.multiple_of(owner * ROWS, ROWS), ROWS)]
        start = pl.multiple_of(owner * ROWS + half * (ROWS // 2), ROWS // 2)
        return pool.at[pl.ds(start, ROWS // 2)]

    pool[pl.ds(pl.multiple_of(seat * ROWS, ROWS), ROWS), :] = vis[...].astype(jnp.bfloat16)
    pl.semaphore_wait(barrier, GROUP - 1 + GROUPS - 1)

    for t in mates:
        remote(
            own_tickets, group_tickets.at[pl.ds(seat, 1)], tick_sems.at[0], tick_sems.at[1], t
        ).start()
    sends = []

    def pass_on(owner, half, send, recv, t):
        copy = remote(block(owner, half), block(owner, half), send, recv, t)
        copy.start()
        sends.append(copy)

    opposite = lax.rem(seat + 2, GROUP)
    pass_on(seat, 0, ring_send.at[0], ring_recv.at[0], partner)
    pass_on(seat, 1, ring_send.at[1], ring_recv.at[1], partner)
    pass_on(seat, None, pair_send.at[0], pair_recv, sibling)

    wait_bytes(group_tickets.at[pl.ds(0, GROUP - 1)], tick_sems.at[1])
    my_rows = pl.ds(pl.multiple_of(base, GROUP), GROUP)
    all_tickets[my_rows, :] = group_tickets[...]
    for t in rows:
        remote(
            group_tickets, all_tickets.at[my_rows], tick_sems.at[2], tick_sems.at[3], t
        ).start()

    loads[6].wait()
    wait_bytes(all_tickets.at[pl.ds(0, (GROUPS - 1) * GROUP)], tick_sems.at[3])
    device = lax.broadcasted_iota(jnp.int32, (ROWS, 1), 0)
    lane = lax.broadcasted_iota(jnp.int32, (1, ROWS), 1)
    everything = all_tickets[...].astype(jnp.float32)
    totals = jnp.sum(everything, axis=1, keepdims=True)
    grand = jnp.sum(totals, axis=0, keepdims=True).astype(jnp.int32)
    z_high, z_low = grand >> SHIFT, grand & (CHAINS - 1)
    jitter = offset_ref[0]

    lines = jnp.sum(
        jnp.where(device // GROUP == lane // GROUP, totals, 0.0), axis=0, keepdims=True
    )
    most = jnp.max(lines, axis=1, keepdims=True).astype(jnp.int32)
    spill_ref[...] = jnp.where(most * ROWS <= cap * grand, 0, 1)

    def point(k):
        return k * z_high + ((k * z_low + jitter) >> SHIFT)

    def count(mask, axis):
        return jnp.sum(jnp.where(mask, 1.0, 0.0), axis=axis, keepdims=True).astype(jnp.int32)

    before = jnp.sum(jnp.where(device < base, totals, 0.0), axis=0, keepdims=True)
    group_first = before.astype(jnp.int32)

    slot_row = lax.broadcasted_iota(jnp.int32, (GROUPS * cap, 1), 0)
    turn = slot_row // cap
    spot = 4 * ((gx + turn // 8) & 3) + ((gz + turn // 2) & 3)
    heir = 8 * spot + 2 * (line + (turn & 1) * (3 - 2 * line)) + core
    first = count(point(lane * ROWS + heir) < group_first, 1)
    place = first + (slot_row & (cap - 1))
    level = jnp.where(place < ROWS, point(place * ROWS + heir), jnp.int32(1 << 30))
    lower = lax.broadcasted_iota(jnp.int32, (ROWS, ROWS), 0) <= lax.broadcasted_iota(
        jnp.int32, (ROWS, ROWS), 1
    )
    mine = group_tickets[...]
    inner = jnp.dot(
        mine.astype(jnp.float32).astype(jnp.bfloat16),
        jnp.where(lower, 1.0, 0.0).astype(jnp.bfloat16),
        preferred_element_type=jnp.float32,
    )
    opened = before
    for d in range(GROUP):
        high = (opened + inner[d : d + 1, :]).astype(jnp.int32)
        low = high - mine[d : d + 1, :]
        onehot[:, d * ROWS : (d + 1) * ROWS] = jnp.where(
            (level >= low) & (level < high), 1.0, 0.0
        ).astype(jnp.bfloat16)
        opened = opened + inner[d : d + 1, ROWS - 1 : ROWS]

    for half in range(2):
        wait_bytes(block(opposite, half), ring_recv.at[half])
        pass_on(opposite, half, pair_send.at[1 + half], pair_recv, sibling)
    wait_bytes(pool.at[pl.ds(0, 2 * ROWS)], pair_recv)

    for part in range(0, GROUPS, ROWS // cap):
        chunk = slice(part * cap, part * cap + ROWS)
        picked = jnp.dot(onehot[chunk, :], pool[...], preferred_element_type=jnp.float32)
        outbox[part : part + ROWS // cap] = picked.reshape(ROWS // cap, cap, 1024).astype(
            jnp.bfloat16
        )
    inbox[pl.ds(group, 1)] = outbox[0:1]
    for i, t in zip(order, rows):
        remote(
            outbox.at[pl.ds(i, 1)], inbox.at[pl.ds(group, 1)], rows_send, rows_recv, t
        ).start()

    loads[2].wait()

    def turn_over(i, carry):
        cols = pl.ds(pl.multiple_of(i * 256, 256), 256)
        for j in range(0, 1024, 256):
            cpl_t[cols, j : j + 256] = cpl[j : j + 256, cols].T
        return carry

    lax.fori_loop(0, 8, turn_over, 0)

    mark = lax.broadcasted_iota(jnp.int32, (1, GROUPS * cap), 1)
    origin = mark // cap
    opens = jnp.sum(
        jnp.where(device < GROUP * origin, totals, 0.0), axis=0, keepdims=True
    ).astype(jnp.int32)
    closes = jnp.sum(
        jnp.where(device < GROUP * origin + GROUP, totals, 0.0), axis=0, keepdims=True
    ).astype(jnp.int32)
    needs = point(device * ROWS + me)
    skipped = count(needs < opens, 0)
    chosen = (device - skipped == (mark & (cap - 1))) & (needs >= opens) & (needs < closes)
    selector = jnp.where(chosen, 1.0, 0.0).astype(jnp.bfloat16)

    for copy in loads[3:6]:
        copy.wait()
    wait_bytes(inbox.at[pl.ds(0, GROUPS - 1)], rows_recv)
    arrived = inbox[...].astype(jnp.float32).reshape(GROUPS * cap, 1024).astype(jnp.bfloat16)
    start = jnp.dot(selector, arrived, preferred_element_type=jnp.float32)
    vis[...] = start
    visb[...] = start.astype(jnp.bfloat16)

    def sweep(s, carry):
        for n in range(0, 2048, 256):
            cols = slice(n, n + 256)
            pre = jnp.dot(visb[...], cpl[:, cols], preferred_element_type=jnp.float32)
            field = pre + hb[:, cols] + nz[s, :, cols].astype(jnp.float32)
            hid[:, cols] = logistic(field).astype(jnp.bfloat16)
        for n in range(0, 1024, 256):
            cols = slice(n, n + 256)
            pre = jnp.dot(hid[...], cpl_t[:, cols], preferred_element_type=jnp.float32)
            new = 0.5 * vis[:, cols] + 0.5 * logistic(pre + vb[:, cols])
            vis[:, cols] = new
            visb[:, cols] = new.astype(jnp.bfloat16)
        return carry

    lax.fori_loop(0, SWEEPS, sweep, 0)
    result = pltpu.make_async_copy(vis, visible_ref, out_sem)
    result.start()

    energy = jnp.sum(vis[...] * vb[...], axis=1, keepdims=True)
    for n in range(0, 2048, 256):
        cols = slice(n, n + 256)
        act = jnp.dot(visb[...], cpl[:, cols], preferred_element_type=jnp.float32) + hb[:, cols]
        soft = jnp.maximum(act, 0.0) + jnp.log(1.0 + jnp.exp(-jnp.abs(act)))
        energy = energy + jnp.sum(soft, axis=1, keepdims=True)
    beta_step = 204.8 / 2048
    log_weight = beta_step * energy
    diagonal = device == lane
    flat = jnp.sum(jnp.where(diagonal, log_weight, 0.0), axis=0, keepdims=True)

    def packed(top, total):
        return jnp.where(lane < ROWS // 2, top, total)

    def merged(ref):
        both = ref[...]
        sums = pltpu.roll(both, ROWS // 2, 1)
        head = lax.broadcasted_iota(jnp.int32, both.shape, 1) < ROWS // 2
        top = jnp.max(jnp.where(head, both, -jnp.inf), axis=(0, 1), keepdims=True)
        one = lax.broadcasted_iota(jnp.int32, both.shape, 1) == 0
        scaled = jnp.where(one, sums * jnp.exp(jnp.where(one, both, top) - top), 0.0)
        return top, jnp.sum(scaled, axis=(0, 1), keepdims=True)

    top = jnp.max(flat, axis=1, keepdims=True)
    total = jnp.sum(jnp.exp(flat - top), axis=1, keepdims=True)
    own_stat[0:1, :] = packed(top, total)
    group_stats[pl.ds(seat, 1), :] = packed(top, total)
    for t in mates:
        remote(
            own_stat.at[pl.ds(0, 1)],
            group_stats.at[pl.ds(seat, 1)],
            stat_sems.at[0],
            stat_sems.at[1],
            t,
        ).start()
    wait_bytes(group_stats.at[pl.ds(0, GROUP - 1)], stat_sems.at[1])
    top, total = merged(group_stats)
    own_stat[8:9, :] = packed(top, total)
    all_stats[pl.ds(group, 1), :] = packed(top, total)
    for t in rows:
        remote(
            own_stat.at[pl.ds(8, 1)],
            all_stats.at[pl.ds(group, 1)],
            stat_sems.at[2],
            stat_sems.at[3],
            t,
        ).start()

    for copy in sends:
        copy.wait_send()
    wait_bytes(group_tickets.at[pl.ds(0, GROUP - 1)], tick_sems.at[0])
    wait_bytes(all_tickets.at[pl.ds(0, (GROUPS - 1) * GROUP)], tick_sems.at[2])
    wait_bytes(outbox.at[pl.ds(1, GROUPS - 1)], rows_send)
    wait_bytes(group_stats.at[pl.ds(0, GROUP - 1)], stat_sems.at[0])

    wait_bytes(all_stats.at[pl.ds(0, GROUPS - 1)], stat_sems.at[3])
    top, total = merged(all_stats)
    weights_ref[...] = jnp.exp(flat - top) * (CHAINS / total)
    ratio_ref[...] = top + jnp.log(total) - jnp.log(jnp.full((1, 1), CHAINS, jnp.float32))
    wait_bytes(all_stats.at[pl.ds(0, GROUPS - 1)], stat_sems.at[2])
    result.wait()


def run(cap, ident, *arrays):
    f32, b16, i32 = jnp.float32, jnp.bfloat16, jnp.int32
    anywhere = pl.BlockSpec(memory_space=pl.ANY)
    dma = pltpu.SemaphoreType.DMA
    return pl.pallas_call(
        functools.partial(step_kernel, cap),
        out_shape=(
            jax.ShapeDtypeStruct((ROWS, 1024), f32),
            jax.ShapeDtypeStruct((1, ROWS), f32),
            jax.ShapeDtypeStruct((1, 1), f32),
            jax.ShapeDtypeStruct((1, 1), i32),
        ),
        in_specs=[anywhere] * 7,
        out_specs=(
            anywhere,
            pl.BlockSpec(memory_space=pltpu.VMEM),
            pl.BlockSpec(memory_space=pltpu.VMEM),
            pl.BlockSpec(memory_space=pltpu.VMEM),
        ),
        scratch_shapes=[
            pltpu.SMEM((1,), i32),
            pltpu.VMEM((1, ROWS), i32),
            pltpu.VMEM((GROUP, ROWS), i32),
            pltpu.VMEM((ROWS, ROWS), i32),
            pltpu.VMEM((ROWS, 1024), f32),
            pltpu.VMEM((GROUP * ROWS, 1024), b16),
            pltpu.VMEM((GROUPS * cap, GROUP * ROWS), b16),
            pltpu.VMEM((GROUPS, cap, 1024), b16),
            pltpu.VMEM((GROUPS, cap, 1024), b16),
            pltpu.VMEM((1024, 2048), b16),
            pltpu.VMEM((2048, 1024), b16),
            pltpu.VMEM((SWEEPS, ROWS, 2048), b16),
            pltpu.VMEM((1, 2048), f32),
            pltpu.VMEM((1, 1024), f32),
            pltpu.VMEM((ROWS, 2048), b16),
            pltpu.VMEM((ROWS, 1024), b16),
            pltpu.VMEM((16, ROWS), f32),
            pltpu.VMEM((GROUP, ROWS), f32),
            pltpu.VMEM((GROUPS, ROWS), f32),
            dma((7,)),
            dma((4,)),
            dma((2,)),
            dma((2,)),
            dma((3,)),
            dma(()),
            dma(()),
            dma(()),
            dma((4,)),
            dma(()),
        ],
        compiler_params=pltpu.CompilerParams(collective_id=ident, has_side_effects=True),
    )(*arrays)


def per_device(states, coupling, vis_bias, hid_bias, noise, tickets, offset):
    arrays = (
        states,
        coupling,
        vis_bias.reshape(1, 1024),
        hid_bias.reshape(1, 2048),
        noise,
        tickets.reshape(1, ROWS),
        offset,
    )
    visible, weights, ratio, spill = run(NARROW, 1, *arrays)
    visible, weights, ratio = lax.cond(
        spill[0, 0] > 0,
        lambda kept: tuple(run(WIDE, 2, *arrays)[:3]),
        lambda kept: kept,
        (visible, weights, ratio),
    )
    return visible, weights.reshape(ROWS), ratio.reshape(())


def solution(mesh):
    both = ("grp", "rep")
    return jax.shard_map(
        per_device,
        mesh=mesh,
        in_specs=(P(both, None), P(), P(), P(), P(None, both, None), P(both), P()),
        out_specs=(P(both, None), P(both), P()),
        check_vma=False,
    )
```

```python
import functools

import jax
import jax.numpy as jnp
from jax import lax
from jax.experimental import pallas as pl
from jax.experimental.pallas import tpu as pltpu
from jax.sharding import PartitionSpec as P

MESH = pl.DeviceIdType.MESH
SWEEPS = 4
ROWS = 128
GROUP = 4
GROUPS = 32
NARROW, WIDE = 8, 16
SHIFT = 14
CHAINS = 1 << SHIFT


def where_is(t):
    return (t // 2, lax.rem(t, 2))


def remote(src, dst, send, recv, t):
    return pltpu.make_async_remote_copy(
        src_ref=src,
        dst_ref=dst,
        send_sem=send,
        recv_sem=recv,
        device_id=where_is(t),
        device_id_type=MESH,
    )


def wait_bytes(ref, sem):
    pltpu.make_async_copy(ref, ref, sem).wait()


def logistic(x):
    return 0.5 * jnp.tanh(0.5 * x) + 0.5


def step_kernel(
    cap,
    states_ref,
    coupling_ref,
    vis_bias_ref,
    hid_bias_ref,
    noise_ref,
    tickets_ref,
    offset_hbm,
    visible_ref,
    small_ref,
    spill_ref,
    offset_ref,
    own_tickets,
    group_tickets,
    all_tickets,
    vis,
    pool,
    onehot,
    outbox,
    inbox,
    cpl,
    cpl_t,
    nz,
    hb,
    vb,
    hid,
    visb,
    own_stat,
    group_stats,
    all_stats,
    load_sems,
    tick_sems,
    ring_send,
    ring_recv,
    pair_send,
    pair_recv,
    rows_send,
    rows_recv,
    stat_sems,
    out_sem,
):
    me = lax.axis_index("grp") * 2 + lax.axis_index("rep")
    core = lax.rem(me, 2)
    seat = lax.rem(me, GROUP)
    line = lax.rem(me // 2, 4)
    group = me // GROUP
    gx, gz = me // 32, lax.rem(me // 8, 4)
    base = me - seat
    sibling = me + 1 - 2 * core
    partner = base + lax.rem(seat + 2, GROUP)
    mates = [base + lax.rem(seat + i, GROUP) for i in range(1, GROUP)]

    def away(i):
        x = lax.rem(gx + i // 8, 4)
        z = lax.rem(gz + i // 2 % 4, 4)
        return 8 * (4 * x + z) + 2 * (line + i % 2 * (3 - 2 * line)) + core

    def hops(i):
        return (0, 1, 2, 1)[i // 8] + (0, 1, 2, 1)[i // 2 % 4] + i % 2

    order = sorted(range(1, GROUPS), key=hops, reverse=True)
    rows = [away(i) for i in order]

    barrier = pltpu.get_barrier_semaphore()
    for t in mates + rows:
        pl.semaphore_signal(barrier, inc=1, device_id=where_is(t), device_id_type=MESH)

    loads = [
        pltpu.make_async_copy(src, dst, load_sems.at[i])
        for i, (src, dst) in enumerate(
            (
                (tickets_ref, own_tickets),
                (states_ref, vis),
                (coupling_ref, cpl),
                (noise_ref, nz),
                (hid_bias_ref, hb),
                (vis_bias_ref, vb),
                (offset_hbm, offset_ref),
            )
        )
    ]
    for copy in loads:
        copy.start()
    loads[0].wait()
    group_tickets[pl.ds(seat, 1), :] = own_tickets[...]
    loads[1].wait()

    def block(owner, half=None):
        if half is None:
            return pool.at[pl.ds(pl.multiple_of(owner * ROWS, ROWS), ROWS)]
        start = pl.multiple_of(owner * ROWS + half * (ROWS // 2), ROWS // 2)
        return pool.at[pl.ds(start, ROWS // 2)]

    pool[pl.ds(pl.multiple_of(seat * ROWS, ROWS), ROWS), :] = vis[...].astype(jnp.bfloat16)
    pl.semaphore_wait(barrier, GROUP - 1 + GROUPS - 1)

    for t in mates:
        remote(
            own_tickets, group_tickets.at[pl.ds(seat, 1)], tick_sems.at[0], tick_sems.at[1], t
        ).start()
    sends = []

    def pass_on(owner, half, send, recv, t):
        copy = remote(block(owner, half), block(owner, half), send, recv, t)
        copy.start()
        sends.append(copy)

    opposite = lax.rem(seat + 2, GROUP)
    pass_on(seat, 0, ring_send.at[0], ring_recv.at[0], partner)
    pass_on(seat, 1, ring_send.at[1], ring_recv.at[1], partner)
    pass_on(seat, None, pair_send.at[0], pair_recv, sibling)

    wait_bytes(group_tickets.at[pl.ds(0, GROUP - 1)], tick_sems.at[1])
    my_rows = pl.ds(pl.multiple_of(base, GROUP), GROUP)
    all_tickets[my_rows, :] = group_tickets[...]
    for t in rows:
        remote(
            group_tickets, all_tickets.at[my_rows], tick_sems.at[2], tick_sems.at[3], t
        ).start()

    loads[6].wait()
    wait_bytes(all_tickets.at[pl.ds(0, (GROUPS - 1) * GROUP)], tick_sems.at[3])
    device = lax.broadcasted_iota(jnp.int32, (ROWS, 1), 0)
    lane = lax.broadcasted_iota(jnp.int32, (1, ROWS), 1)
    everything = all_tickets[...].astype(jnp.float32)
    totals = jnp.sum(everything, axis=1, keepdims=True)
    grand = jnp.sum(totals, axis=0, keepdims=True).astype(jnp.int32)
    z_high, z_low = grand >> SHIFT, grand & (CHAINS - 1)
    jitter = offset_ref[...]

    lines = jnp.sum(
        jnp.where(device // GROUP == lane // GROUP, totals, 0.0), axis=0, keepdims=True
    )
    most = jnp.max(lines, axis=1, keepdims=True).astype(jnp.int32)
    spill_ref[0, 0] = jnp.where(most * ROWS <= cap * grand, 0, 1)[0, 0]

    def point(k):
        return k * z_high + ((k * z_low + jitter) >> SHIFT)

    def count(mask, axis):
        return jnp.sum(jnp.where(mask, 1.0, 0.0), axis=axis, keepdims=True).astype(jnp.int32)

    before = jnp.sum(jnp.where(device < base, totals, 0.0), axis=0, keepdims=True)
    group_first = before.astype(jnp.int32)

    slot_row = lax.broadcasted_iota(jnp.int32, (GROUPS * cap, 1), 0)
    turn = slot_row // cap
    spot = 4 * ((gx + turn // 8) & 3) + ((gz + turn // 2) & 3)
    heir = 8 * spot + 2 * (line + (turn & 1) * (3 - 2 * line)) + core
    first = count(point(lane * ROWS + heir) < group_first, 1)
    place = first + (slot_row & (cap - 1))
    level = jnp.where(place < ROWS, point(place * ROWS + heir), jnp.int32(1 << 30))
    lower = lax.broadcasted_iota(jnp.int32, (ROWS, ROWS), 0) <= lax.broadcasted_iota(
        jnp.int32, (ROWS, ROWS), 1
    )
    mine = group_tickets[...]
    inner = jnp.dot(
        mine.astype(jnp.float32).astype(jnp.bfloat16),
        jnp.where(lower, 1.0, 0.0).astype(jnp.bfloat16),
        preferred_element_type=jnp.float32,
    )
    opened = before
    for d in range(GROUP):
        high = (opened + inner[d : d + 1, :]).astype(jnp.int32)
        low = high - mine[d : d + 1, :]
        onehot[:, d * ROWS : (d + 1) * ROWS] = jnp.where(
            (level >= low) & (level < high), 1.0, 0.0
        ).astype(jnp.bfloat16)
        opened = opened + inner[d : d + 1, ROWS - 1 : ROWS]

    for half in range(2):
        wait_bytes(block(opposite, half), ring_recv.at[half])
        pass_on(opposite, half, pair_send.at[1 + half], pair_recv, sibling)
    wait_bytes(pool.at[pl.ds(0, 2 * ROWS)], pair_recv)

    for part in range(0, GROUPS, ROWS // cap):
        chunk = slice(part * cap, part * cap + ROWS)
        picked = jnp.dot(onehot[chunk, :], pool[...], preferred_element_type=jnp.float32)
        outbox[part : part + ROWS // cap] = picked.reshape(ROWS // cap, cap, 1024).astype(
            jnp.bfloat16
        )
    inbox[pl.ds(group, 1)] = outbox[0:1]
    for i, t in zip(order, rows):
        remote(
            outbox.at[pl.ds(i, 1)], inbox.at[pl.ds(group, 1)], rows_send, rows_recv, t
        ).start()

    loads[2].wait()

    def turn_over(i, carry):
        cols = pl.ds(pl.multiple_of(i * 256, 256), 256)
        for j in range(0, 1024, 256):
            cpl_t[cols, j : j + 256] = cpl[j : j + 256, cols].T
        return carry

    lax.fori_loop(0, 8, turn_over, 0)

    mark = lax.broadcasted_iota(jnp.int32, (1, GROUPS * cap), 1)
    origin = mark // cap
    opens = jnp.sum(
        jnp.where(device < GROUP * origin, totals, 0.0), axis=0, keepdims=True
    ).astype(jnp.int32)
    closes = jnp.sum(
        jnp.where(device < GROUP * origin + GROUP, totals, 0.0), axis=0, keepdims=True
    ).astype(jnp.int32)
    needs = point(device * ROWS + me)
    skipped = count(needs < opens, 0)
    chosen = (device - skipped == (mark & (cap - 1))) & (needs >= opens) & (needs < closes)
    selector = jnp.where(chosen, 1.0, 0.0).astype(jnp.bfloat16)

    for copy in loads[3:6]:
        copy.wait()
    wait_bytes(inbox.at[pl.ds(0, GROUPS - 1)], rows_recv)
    arrived = inbox[...].astype(jnp.float32).reshape(GROUPS * cap, 1024).astype(jnp.bfloat16)
    start = jnp.dot(selector, arrived, preferred_element_type=jnp.float32)
    vis[...] = start
    visb[...] = start.astype(jnp.bfloat16)

    def sweep(s, carry):
        for n in range(0, 2048, 256):
            cols = slice(n, n + 256)
            pre = jnp.dot(visb[...], cpl[:, cols], preferred_element_type=jnp.float32)
            field = pre + hb[:, cols] + nz[s, :, cols].astype(jnp.float32)
            hid[:, cols] = logistic(field).astype(jnp.bfloat16)
        for n in range(0, 1024, 256):
            cols = slice(n, n + 256)
            pre = jnp.dot(hid[...], cpl_t[:, cols], preferred_element_type=jnp.float32)
            new = 0.5 * vis[:, cols] + 0.5 * logistic(pre + vb[:, cols])
            vis[:, cols] = new
            visb[:, cols] = new.astype(jnp.bfloat16)
        return carry

    if cap == NARROW:
        for s in range(SWEEPS):
            sweep(s, 0)
    else:
        lax.fori_loop(0, SWEEPS, sweep, 0)
    result = pltpu.make_async_copy(vis, visible_ref, out_sem)
    result.start()

    energy = jnp.sum(vis[...] * vb[...], axis=1, keepdims=True)
    for n in range(0, 2048, 256):
        cols = slice(n, n + 256)
        act = jnp.dot(visb[...], cpl[:, cols], preferred_element_type=jnp.float32) + hb[:, cols]
        soft = jnp.maximum(act, 0.0) + jnp.log(1.0 + jnp.exp(-jnp.abs(act)))
        energy = energy + jnp.sum(soft, axis=1, keepdims=True)
    beta_step = 204.8 / 2048
    log_weight = beta_step * energy
    diagonal = device == lane
    flat = jnp.sum(jnp.where(diagonal, log_weight, 0.0), axis=0, keepdims=True)

    def packed(top, total):
        return jnp.where(lane < ROWS // 2, top, total)

    def merged(ref):
        both = ref[...]
        sums = pltpu.roll(both, ROWS // 2, 1)
        head = lax.broadcasted_iota(jnp.int32, both.shape, 1) < ROWS // 2
        top = jnp.max(jnp.where(head, both, -jnp.inf), axis=(0, 1), keepdims=True)
        one = lax.broadcasted_iota(jnp.int32, both.shape, 1) == 0
        scaled = jnp.where(one, sums * jnp.exp(jnp.where(one, both, top) - top), 0.0)
        return top, jnp.sum(scaled, axis=(0, 1), keepdims=True)

    top = jnp.max(flat, axis=1, keepdims=True)
    total = jnp.sum(jnp.exp(flat - top), axis=1, keepdims=True)
    own_stat[0:1, :] = packed(top, total)
    group_stats[pl.ds(seat, 1), :] = packed(top, total)
    for t in mates:
        remote(
            own_stat.at[pl.ds(0, 1)],
            group_stats.at[pl.ds(seat, 1)],
            stat_sems.at[0],
            stat_sems.at[1],
            t,
        ).start()
    wait_bytes(group_stats.at[pl.ds(0, GROUP - 1)], stat_sems.at[1])
    top, total = merged(group_stats)
    own_stat[8:9, :] = packed(top, total)
    all_stats[pl.ds(group, 1), :] = packed(top, total)
    for t in rows:
        remote(
            own_stat.at[pl.ds(8, 1)],
            all_stats.at[pl.ds(group, 1)],
            stat_sems.at[2],
            stat_sems.at[3],
            t,
        ).start()

    for copy in sends:
        copy.wait_send()
    wait_bytes(group_tickets.at[pl.ds(0, GROUP - 1)], tick_sems.at[0])
    wait_bytes(all_tickets.at[pl.ds(0, (GROUPS - 1) * GROUP)], tick_sems.at[2])
    wait_bytes(outbox.at[pl.ds(1, GROUPS - 1)], rows_send)
    wait_bytes(group_stats.at[pl.ds(0, GROUP - 1)], stat_sems.at[0])

    wait_bytes(all_stats.at[pl.ds(0, GROUPS - 1)], stat_sems.at[3])
    top, total = merged(all_stats)
    small_ref[:, :ROWS] = jnp.exp(flat - top) * (CHAINS / total)
    ratio = top + jnp.log(total) - jnp.log(jnp.full((1, 1), CHAINS, jnp.float32))
    small_ref[:, ROWS:] = jnp.broadcast_to(ratio, (1, ROWS))
    wait_bytes(all_stats.at[pl.ds(0, GROUPS - 1)], stat_sems.at[2])
    result.wait()


def finish_kernel(visible, small, visible_out, weights_out, ratio_out, ratio, sems):
    ratio[...] = small[:, ROWS : ROWS + 1]
    copies = [
        pltpu.make_async_copy(src, dst, sems.at[i])
        for i, (src, dst) in enumerate(
            ((visible, visible_out), (small.at[:, pl.ds(0, ROWS)], weights_out), (ratio, ratio_out))
        )
    ]
    for copy in copies:
        copy.start()
    for copy in copies:
        copy.wait()


def run(cap, ident, *arrays):
    f32, b16, i32 = jnp.float32, jnp.bfloat16, jnp.int32
    anywhere = pl.BlockSpec(memory_space=pl.ANY)
    dma = pltpu.SemaphoreType.DMA
    return pl.pallas_call(
        functools.partial(step_kernel, cap),
        out_shape=(
            jax.ShapeDtypeStruct((ROWS, 1024), f32),
            jax.ShapeDtypeStruct((1, 2 * ROWS), f32),
            jax.ShapeDtypeStruct((1, 1), i32),
        ),
        in_specs=[anywhere] * 7,
        out_specs=(
            anywhere,
            pl.BlockSpec(memory_space=pltpu.VMEM),
            pl.BlockSpec(memory_space=pltpu.SMEM),
        ),
        scratch_shapes=[
            pltpu.VMEM((1, 1), i32),
            pltpu.VMEM((1, ROWS), i32),
            pltpu.VMEM((GROUP, ROWS), i32),
            pltpu.VMEM((ROWS, ROWS), i32),
            pltpu.VMEM((ROWS, 1024), f32),
            pltpu.VMEM((GROUP * ROWS, 1024), b16),
            pltpu.VMEM((GROUPS * cap, GROUP * ROWS), b16),
            pltpu.VMEM((GROUPS, cap, 1024), b16),
            pltpu.VMEM((GROUPS, cap, 1024), b16),
            pltpu.VMEM((1024, 2048), b16),
            pltpu.VMEM((2048, 1024), b16),
            pltpu.VMEM((SWEEPS, ROWS, 2048), b16),
            pltpu.VMEM((1, 2048), f32),
            pltpu.VMEM((1, 1024), f32),
            pltpu.VMEM((ROWS, 2048), b16),
            pltpu.VMEM((ROWS, 1024), b16),
            pltpu.VMEM((16, ROWS), f32),
            pltpu.VMEM((GROUP, ROWS), f32),
            pltpu.VMEM((GROUPS, ROWS), f32),
            dma((7,)),
            dma((4,)),
            dma((2,)),
            dma((2,)),
            dma((3,)),
            dma(()),
            dma(()),
            dma(()),
            dma((4,)),
            dma(()),
        ],
        compiler_params=pltpu.CompilerParams(collective_id=ident, has_side_effects=True),
    )(*arrays)


def per_device(states, coupling, vis_bias, hid_bias, noise, tickets, offset):
    arrays = (
        states,
        coupling,
        vis_bias.reshape(1, 1024),
        hid_bias.reshape(1, 2048),
        noise,
        tickets.reshape(1, ROWS),
        offset.reshape(1, 1),
    )
    visible, small, spill = run(NARROW, 1, *arrays)
    visible, small = lax.cond(
        spill[0, 0] > 0,
        lambda kept: tuple(run(WIDE, 2, *arrays)[:2]),
        lambda kept: kept,
        (visible, small),
    )
    inside = pl.BlockSpec(memory_space=pltpu.VMEM)
    outside = pl.BlockSpec(memory_space=pl.ANY)
    visible, weights, ratio = pl.pallas_call(
        finish_kernel,
        out_shape=tuple(
            jax.ShapeDtypeStruct(shape, jnp.float32) for shape in ((ROWS, 1024), (1, ROWS), (1, 1))
        ),
        in_specs=[inside] * 2,
        out_specs=[outside] * 3,
        scratch_shapes=[pltpu.VMEM((1, 1), jnp.float32), pltpu.SemaphoreType.DMA((3,))],
    )(visible, small)
    return visible, weights.reshape(ROWS), ratio.reshape(())


def solution(mesh):
    both = ("grp", "rep")
    return jax.shard_map(
        per_device,
        mesh=mesh,
        in_specs=(P(both, None), P(), P(), P(), P(None, both, None), P(both), P()),
        out_specs=(P(both, None), P(both), P()),
        check_vma=False,
    )
```

```python
import functools

import jax
import jax.numpy as jnp
from jax import lax
from jax.experimental import pallas as pl
from jax.experimental.pallas import tpu as pltpu
from jax.sharding import PartitionSpec as P

MESH = pl.DeviceIdType.MESH
SWEEPS = 4
ROWS = 128
GROUP = 4
GROUPS = 32
NARROW, WIDE = 8, 16
SHIFT = 14
CHAINS = 1 << SHIFT


def where_is(t):
    return (t // 2, lax.rem(t, 2))


def remote(src, dst, send, recv, t):
    return pltpu.make_async_remote_copy(
        src_ref=src,
        dst_ref=dst,
        send_sem=send,
        recv_sem=recv,
        device_id=where_is(t),
        device_id_type=MESH,
    )


def wait_bytes(ref, sem):
    pltpu.make_async_copy(ref, ref, sem).wait()


def logistic(x):
    return 0.5 * jnp.tanh(0.5 * x) + 0.5


def step_kernel(
    cap,
    states_ref,
    coupling_ref,
    vis_bias_ref,
    hid_bias_ref,
    noise_ref,
    tickets_ref,
    offset_hbm,
    visible_ref,
    small_ref,
    spill_ref,
    offset_ref,
    own_tickets,
    group_tickets,
    all_tickets,
    vis,
    pool,
    onehot,
    outbox,
    inbox,
    cpl,
    cpl_t,
    nz,
    hb,
    vb,
    hid,
    visb,
    own_stat,
    all_stats,
    load_sems,
    tick_sems,
    ring_send,
    ring_recv,
    pair_send,
    pair_recv,
    rows_send,
    rows_recv,
    stat_sems,
    out_sem,
):
    me = lax.axis_index("grp") * 2 + lax.axis_index("rep")
    core = lax.rem(me, 2)
    seat = lax.rem(me, GROUP)
    line = lax.rem(me // 2, 4)
    group = me // GROUP
    gx, gz = me // 32, lax.rem(me // 8, 4)
    base = me - seat
    sibling = me + 1 - 2 * core
    partner = base + lax.rem(seat + 2, GROUP)
    mates = [base + lax.rem(seat + i, GROUP) for i in range(1, GROUP)]

    def away(i):
        x = lax.rem(gx + i // 8, 4)
        z = lax.rem(gz + i // 2 % 4, 4)
        return 8 * (4 * x + z) + 2 * (line + i % 2 * (3 - 2 * line)) + core

    def hops(i):
        return (0, 1, 2, 1)[i // 8] + (0, 1, 2, 1)[i // 2 % 4] + i % 2

    order = sorted(range(1, GROUPS), key=hops, reverse=True)
    rows = [away(i) for i in order]

    def everyone():
        far = (0, 1, 2, 1)
        steps = [
            (x, z, y, c) for x in range(4) for z in range(4) for y in range(4) for c in range(2)
        ][1:]
        steps.sort(key=lambda d: (-far[d[0]] - far[d[1]] - far[d[2]], -d[3]))
        xs = [16 * lax.rem(gx + i, 4) for i in range(4)]
        zs = [4 * lax.rem(gz + i, 4) for i in range(4)]
        ys = [lax.rem(line + i, 4) for i in range(4)]
        cs = [core, 1 - core]
        return [(xs[x] + zs[z] + ys[y], cs[c]) for x, z, y, c in steps]

    barrier = pltpu.get_barrier_semaphore()
    for t in mates + rows:
        pl.semaphore_signal(barrier, inc=1, device_id=where_is(t), device_id_type=MESH)

    loads = [
        pltpu.make_async_copy(src, dst, load_sems.at[i])
        for i, (src, dst) in enumerate(
            (
                (tickets_ref, own_tickets),
                (states_ref, vis),
                (coupling_ref, cpl),
                (noise_ref, nz),
                (hid_bias_ref, hb),
                (vis_bias_ref, vb),
                (offset_hbm, offset_ref),
            )
        )
    ]
    for copy in loads:
        copy.start()
    loads[0].wait()
    group_tickets[pl.ds(seat, 1), :] = own_tickets[...]
    loads[1].wait()

    def block(owner, half=None):
        if half is None:
            return pool.at[pl.ds(pl.multiple_of(owner * ROWS, ROWS), ROWS)]
        start = pl.multiple_of(owner * ROWS + half * (ROWS // 2), ROWS // 2)
        return pool.at[pl.ds(start, ROWS // 2)]

    pool[pl.ds(pl.multiple_of(seat * ROWS, ROWS), ROWS), :] = vis[...].astype(jnp.bfloat16)
    pl.semaphore_wait(barrier, GROUP - 1 + GROUPS - 1)

    for t in mates:
        remote(
            own_tickets, group_tickets.at[pl.ds(seat, 1)], tick_sems.at[0], tick_sems.at[1], t
        ).start()
    sends = []

    def pass_on(owner, half, send, recv, t):
        copy = remote(block(owner, half), block(owner, half), send, recv, t)
        copy.start()
        sends.append(copy)

    opposite = lax.rem(seat + 2, GROUP)
    pass_on(seat, 0, ring_send.at[0], ring_recv.at[0], partner)
    pass_on(seat, 1, ring_send.at[1], ring_recv.at[1], partner)
    pass_on(seat, None, pair_send.at[0], pair_recv, sibling)

    wait_bytes(group_tickets.at[pl.ds(0, GROUP - 1)], tick_sems.at[1])
    my_rows = pl.ds(pl.multiple_of(base, GROUP), GROUP)
    all_tickets[my_rows, :] = group_tickets[...]
    for t in rows:
        remote(
            group_tickets, all_tickets.at[my_rows], tick_sems.at[2], tick_sems.at[3], t
        ).start()

    loads[6].wait()
    wait_bytes(all_tickets.at[pl.ds(0, (GROUPS - 1) * GROUP)], tick_sems.at[3])
    device = lax.broadcasted_iota(jnp.int32, (ROWS, 1), 0)
    lane = lax.broadcasted_iota(jnp.int32, (1, ROWS), 1)
    everything = all_tickets[...].astype(jnp.float32)
    totals = jnp.sum(everything, axis=1, keepdims=True)
    grand = jnp.sum(totals, axis=0, keepdims=True).astype(jnp.int32)
    z_high, z_low = grand >> SHIFT, grand & (CHAINS - 1)
    jitter = offset_ref[...]

    lines = jnp.sum(
        jnp.where(device // GROUP == lane // GROUP, totals, 0.0), axis=0, keepdims=True
    )
    most = jnp.max(lines, axis=1, keepdims=True).astype(jnp.int32)
    spill_ref[0, 0] = jnp.where(most * ROWS <= cap * grand, 0, 1)[0, 0]

    def point(k):
        return k * z_high + ((k * z_low + jitter) >> SHIFT)

    def count(mask, axis):
        return jnp.sum(jnp.where(mask, 1.0, 0.0), axis=axis, keepdims=True).astype(jnp.int32)

    before = jnp.sum(jnp.where(device < base, totals, 0.0), axis=0, keepdims=True)
    group_first = before.astype(jnp.int32)

    slot_row = lax.broadcasted_iota(jnp.int32, (GROUPS * cap, 1), 0)
    turn = slot_row // cap
    spot = 4 * ((gx + turn // 8) & 3) + ((gz + turn // 2) & 3)
    heir = 8 * spot + 2 * (line + (turn & 1) * (3 - 2 * line)) + core
    first = count(point(lane * ROWS + heir) < group_first, 1)
    place = first + (slot_row & (cap - 1))
    level = jnp.where(place < ROWS, point(place * ROWS + heir), jnp.int32(1 << 30))
    lower = lax.broadcasted_iota(jnp.int32, (ROWS, ROWS), 0) <= lax.broadcasted_iota(
        jnp.int32, (ROWS, ROWS), 1
    )
    mine = group_tickets[...]
    inner = jnp.dot(
        mine.astype(jnp.float32).astype(jnp.bfloat16),
        jnp.where(lower, 1.0, 0.0).astype(jnp.bfloat16),
        preferred_element_type=jnp.float32,
    )
    opened = before
    for d in range(GROUP):
        high = (opened + inner[d : d + 1, :]).astype(jnp.int32)
        low = high - mine[d : d + 1, :]
        onehot[:, d * ROWS : (d + 1) * ROWS] = jnp.where(
            (level >= low) & (level < high), 1.0, 0.0
        ).astype(jnp.bfloat16)
        opened = opened + inner[d : d + 1, ROWS - 1 : ROWS]

    for half in range(2):
        wait_bytes(block(opposite, half), ring_recv.at[half])
        pass_on(opposite, half, pair_send.at[1 + half], pair_recv, sibling)
    wait_bytes(pool.at[pl.ds(0, 2 * ROWS)], pair_recv)

    for part in range(0, GROUPS, ROWS // cap):
        chunk = slice(part * cap, part * cap + ROWS)
        picked = jnp.dot(onehot[chunk, :], pool[...], preferred_element_type=jnp.float32)
        outbox[part : part + ROWS // cap] = picked.reshape(ROWS // cap, cap, 1024).astype(
            jnp.bfloat16
        )
    inbox[pl.ds(group, 1)] = outbox[0:1]
    for i, t in zip(order, rows):
        remote(
            outbox.at[pl.ds(i, 1)], inbox.at[pl.ds(group, 1)], rows_send, rows_recv, t
        ).start()

    loads[2].wait()

    def turn_over(i, carry):
        cols = pl.ds(pl.multiple_of(i * 256, 256), 256)
        for j in range(0, 1024, 256):
            cpl_t[cols, j : j + 256] = cpl[j : j + 256, cols].T
        return carry

    lax.fori_loop(0, 8, turn_over, 0)

    mark = lax.broadcasted_iota(jnp.int32, (1, GROUPS * cap), 1)
    origin = mark // cap
    opens = jnp.sum(
        jnp.where(device < GROUP * origin, totals, 0.0), axis=0, keepdims=True
    ).astype(jnp.int32)
    closes = jnp.sum(
        jnp.where(device < GROUP * origin + GROUP, totals, 0.0), axis=0, keepdims=True
    ).astype(jnp.int32)
    needs = point(device * ROWS + me)
    skipped = count(needs < opens, 0)
    chosen = (device - skipped == (mark & (cap - 1))) & (needs >= opens) & (needs < closes)
    selector = jnp.where(chosen, 1.0, 0.0).astype(jnp.bfloat16)

    for copy in loads[3:6]:
        copy.wait()
    wait_bytes(inbox.at[pl.ds(0, GROUPS - 1)], rows_recv)
    arrived = inbox[...].astype(jnp.float32).reshape(GROUPS * cap, 1024).astype(jnp.bfloat16)
    start = jnp.dot(selector, arrived, preferred_element_type=jnp.float32)
    vis[...] = start
    visb[...] = start.astype(jnp.bfloat16)

    def sweep(s, carry):
        for n in range(0, 2048, 256):
            cols = slice(n, n + 256)
            pre = jnp.dot(visb[...], cpl[:, cols], preferred_element_type=jnp.float32)
            field = pre + hb[:, cols] + nz[s, :, cols].astype(jnp.float32)
            hid[:, cols] = logistic(field).astype(jnp.bfloat16)
        for n in range(0, 1024, 256):
            cols = slice(n, n + 256)
            pre = jnp.dot(hid[...], cpl_t[:, cols], preferred_element_type=jnp.float32)
            new = 0.5 * vis[:, cols] + 0.5 * logistic(pre + vb[:, cols])
            vis[:, cols] = new
            visb[:, cols] = new.astype(jnp.bfloat16)
        return carry

    if cap == NARROW:
        for s in range(SWEEPS):
            sweep(s, 0)
    else:
        lax.fori_loop(0, SWEEPS, sweep, 0)
    result = pltpu.make_async_copy(vis, visible_ref, out_sem)
    result.start()

    energy = jnp.sum(vis[...] * vb[...], axis=1, keepdims=True)
    for n in range(0, 2048, 256):
        cols = slice(n, n + 256)
        act = jnp.dot(visb[...], cpl[:, cols], preferred_element_type=jnp.float32) + hb[:, cols]
        soft = jnp.maximum(act, 0.0) + jnp.log(1.0 + jnp.exp(-jnp.abs(act)))
        energy = energy + jnp.sum(soft, axis=1, keepdims=True)
    beta_step = 204.8 / 2048
    log_weight = beta_step * energy
    diagonal = device == lane
    flat = jnp.sum(jnp.where(diagonal, log_weight, 0.0), axis=0, keepdims=True)

    def packed(top, total):
        return jnp.where(lane < ROWS // 2, top, total)

    def merged(ref):
        both = ref[...]
        sums = pltpu.roll(both, ROWS // 2, 1)
        head = lax.broadcasted_iota(jnp.int32, both.shape, 1) < ROWS // 2
        top = jnp.max(jnp.where(head, both, -jnp.inf), axis=(0, 1), keepdims=True)
        one = lax.broadcasted_iota(jnp.int32, both.shape, 1) == 0
        scaled = jnp.where(one, sums * jnp.exp(jnp.where(one, both, top) - top), 0.0)
        return top, jnp.sum(scaled, axis=(0, 1), keepdims=True)

    top = jnp.max(flat, axis=1, keepdims=True)
    total = jnp.sum(jnp.exp(flat - top), axis=1, keepdims=True)
    own_stat[...] = packed(top, total)
    all_stats[pl.ds(me, 1), :] = packed(top, total)
    for t in everyone():
        pltpu.make_async_remote_copy(
            src_ref=own_stat,
            dst_ref=all_stats.at[pl.ds(me, 1)],
            send_sem=stat_sems.at[0],
            recv_sem=stat_sems.at[1],
            device_id=t,
            device_id_type=MESH,
        ).start()

    for copy in sends:
        copy.wait_send()
    wait_bytes(group_tickets.at[pl.ds(0, GROUP - 1)], tick_sems.at[0])
    wait_bytes(all_tickets.at[pl.ds(0, (GROUPS - 1) * GROUP)], tick_sems.at[2])
    wait_bytes(outbox.at[pl.ds(1, GROUPS - 1)], rows_send)

    wait_bytes(all_stats.at[pl.ds(0, ROWS - 1)], stat_sems.at[1])
    top, total = merged(all_stats)
    small_ref[:, :ROWS] = jnp.exp(flat - top) * (CHAINS / total)
    ratio = top + jnp.log(total) - jnp.log(jnp.full((1, 1), CHAINS, jnp.float32))
    small_ref[:, ROWS:] = jnp.broadcast_to(ratio, (1, ROWS))
    wait_bytes(all_stats.at[pl.ds(0, ROWS - 1)], stat_sems.at[0])
    result.wait()


def finish_kernel(visible, small, visible_out, weights_out, ratio_out, ratio, sems):
    ratio[...] = small[:, ROWS : ROWS + 1]
    copies = [
        pltpu.make_async_copy(src, dst, sems.at[i])
        for i, (src, dst) in enumerate(
            ((visible, visible_out), (small.at[:, pl.ds(0, ROWS)], weights_out), (ratio, ratio_out))
        )
    ]
    for copy in copies:
        copy.start()
    for copy in copies:
        copy.wait()


def run(cap, ident, *arrays):
    f32, b16, i32 = jnp.float32, jnp.bfloat16, jnp.int32
    anywhere = pl.BlockSpec(memory_space=pl.ANY)
    dma = pltpu.SemaphoreType.DMA
    return pl.pallas_call(
        functools.partial(step_kernel, cap),
        out_shape=(
            jax.ShapeDtypeStruct((ROWS, 1024), f32),
            jax.ShapeDtypeStruct((1, 2 * ROWS), f32),
            jax.ShapeDtypeStruct((1, 1), i32),
        ),
        in_specs=[anywhere] * 7,
        out_specs=(
            anywhere,
            pl.BlockSpec(memory_space=pltpu.VMEM),
            pl.BlockSpec(memory_space=pltpu.SMEM),
        ),
        scratch_shapes=[
            pltpu.VMEM((1, 1), i32),
            pltpu.VMEM((1, ROWS), i32),
            pltpu.VMEM((GROUP, ROWS), i32),
            pltpu.VMEM((ROWS, ROWS), i32),
            pltpu.VMEM((ROWS, 1024), f32),
            pltpu.VMEM((GROUP * ROWS, 1024), b16),
            pltpu.VMEM((GROUPS * cap, GROUP * ROWS), b16),
            pltpu.VMEM((GROUPS, cap, 1024), b16),
            pltpu.VMEM((GROUPS, cap, 1024), b16),
            pltpu.VMEM((1024, 2048), b16),
            pltpu.VMEM((2048, 1024), b16),
            pltpu.VMEM((SWEEPS, ROWS, 2048), b16),
            pltpu.VMEM((1, 2048), f32),
            pltpu.VMEM((1, 1024), f32),
            pltpu.VMEM((ROWS, 2048), b16),
            pltpu.VMEM((ROWS, 1024), b16),
            pltpu.VMEM((1, ROWS), f32),
            pltpu.VMEM((ROWS, ROWS), f32),
            dma((7,)),
            dma((4,)),
            dma((2,)),
            dma((2,)),
            dma((3,)),
            dma(()),
            dma(()),
            dma(()),
            dma((2,)),
            dma(()),
        ],
        compiler_params=pltpu.CompilerParams(collective_id=ident, has_side_effects=True),
    )(*arrays)


def per_device(states, coupling, vis_bias, hid_bias, noise, tickets, offset):
    arrays = (
        states,
        coupling,
        vis_bias.reshape(1, 1024),
        hid_bias.reshape(1, 2048),
        noise,
        tickets.reshape(1, ROWS),
        offset.reshape(1, 1),
    )
    visible, small, spill = run(NARROW, 1, *arrays)
    visible, small = lax.cond(
        spill[0, 0] > 0,
        lambda kept: tuple(run(WIDE, 2, *arrays)[:2]),
        lambda kept: kept,
        (visible, small),
    )
    inside = pl.BlockSpec(memory_space=pltpu.VMEM)
    outside = pl.BlockSpec(memory_space=pl.ANY)
    visible, weights, ratio = pl.pallas_call(
        finish_kernel,
        out_shape=tuple(
            jax.ShapeDtypeStruct(shape, jnp.float32) for shape in ((ROWS, 1024), (1, ROWS), (1, 1))
        ),
        in_specs=[inside] * 2,
        out_specs=[outside] * 3,
        scratch_shapes=[pltpu.VMEM((1, 1), jnp.float32), pltpu.SemaphoreType.DMA((3,))],
    )(visible, small)
    return visible, weights.reshape(ROWS), ratio.reshape(())


def solution(mesh):
    both = ("grp", "rep")
    return jax.shard_map(
        per_device,
        mesh=mesh,
        in_specs=(P(both, None), P(), P(), P(), P(None, both, None), P(both), P()),
        out_specs=(P(both, None), P(both), P()),
        check_vma=False,
    )
```

```python
import functools

import jax
import jax.numpy as jnp
from jax import lax
from jax.experimental import pallas as pl
from jax.experimental.pallas import tpu as pltpu
from jax.sharding import PartitionSpec as P

MESH = pl.DeviceIdType.MESH
SWEEPS = 4
ROWS = 128
GROUP = 4
GROUPS = 32
LINE = 8
NARROW, WIDE = 8, 16
SHIFT = 14
CHAINS = 1 << SHIFT


def where_is(t):
    return (t // 2, lax.rem(t, 2))


def remote(src, dst, send, recv, t):
    return pltpu.make_async_remote_copy(
        src_ref=src,
        dst_ref=dst,
        send_sem=send,
        recv_sem=recv,
        device_id=where_is(t),
        device_id_type=MESH,
    )


def wait_bytes(ref, sem):
    pltpu.make_async_copy(ref, ref, sem).wait()


def logistic(x):
    return 0.5 * jnp.tanh(0.5 * x) + 0.5


def step_kernel(
    cap,
    states_ref,
    coupling_ref,
    vis_bias_ref,
    hid_bias_ref,
    noise_ref,
    tickets_ref,
    offset_hbm,
    visible_ref,
    small_ref,
    spill_ref,
    offset_ref,
    own_tickets,
    line_tickets,
    all_tickets,
    vis,
    pool,
    onehot,
    outbox,
    inbox,
    cpl,
    cpl_t,
    nz,
    hb,
    vb,
    hid,
    visb,
    own_stat,
    all_stats,
    load_sems,
    tick_sems,
    ring_send,
    ring_recv,
    pair_send,
    pair_recv,
    rows_send,
    rows_recv,
    stat_sems,
    out_sem,
):
    me = lax.axis_index("grp") * 2 + lax.axis_index("rep")
    core = lax.rem(me, 2)
    seat = lax.rem(me, GROUP)
    line = lax.rem(me // 2, 4)
    group = me // GROUP
    gx, gz = me // 32, lax.rem(me // 8, 4)
    base = me - seat
    sibling = me + 1 - 2 * core
    partner = base + lax.rem(seat + 2, GROUP)
    desk = lax.rem(me, LINE)
    front = me - desk
    mates = [front + lax.rem(desk + i, LINE) for i in range(1, LINE)]
    far = (0, 1, 2, 1)
    planes = [
        LINE * (4 * lax.rem(gx + x, 4) + lax.rem(gz + z, 4)) + desk
        for x, z in sorted(
            ((x, z) for x in range(4) for z in range(4) if x + z), key=lambda d: -far[d[0]] - far[d[1]]
        )
    ]

    def away(i):
        x = lax.rem(gx + i // 8, 4)
        z = lax.rem(gz + i // 2 % 4, 4)
        return 8 * (4 * x + z) + 2 * (line + i % 2 * (3 - 2 * line)) + core

    def hops(i):
        return (0, 1, 2, 1)[i // 8] + (0, 1, 2, 1)[i // 2 % 4] + i % 2

    order = sorted(range(1, GROUPS), key=hops, reverse=True)

    def everyone():
        steps = [
            (x, z, y, c) for x in range(4) for z in range(4) for y in range(4) for c in range(2)
        ][1:]
        steps.sort(key=lambda d: (-far[d[0]] - far[d[1]] - far[d[2]], -d[3]))
        xs = [16 * lax.rem(gx + i, 4) for i in range(4)]
        zs = [4 * lax.rem(gz + i, 4) for i in range(4)]
        ys = [lax.rem(line + i, 4) for i in range(4)]
        cs = [core, 1 - core]
        return [(xs[x] + zs[z] + ys[y], cs[c]) for x, z, y, c in steps]

    barrier = pltpu.get_barrier_semaphore()
    for t in planes + mates:
        pl.semaphore_signal(barrier, inc=1, device_id=where_is(t), device_id_type=MESH)

    loads = [
        pltpu.make_async_copy(src, dst, load_sems.at[i])
        for i, (src, dst) in enumerate(
            (
                (tickets_ref, own_tickets),
                (states_ref, vis),
                (coupling_ref, cpl),
                (noise_ref, nz),
                (hid_bias_ref, hb),
                (vis_bias_ref, vb),
                (offset_hbm, offset_ref),
            )
        )
    ]
    for copy in loads:
        copy.start()
    loads[0].wait()
    line_tickets[pl.ds(desk, 1), :] = own_tickets[...]
    loads[1].wait()

    def block(owner, half=None):
        if half is None:
            return pool.at[pl.ds(pl.multiple_of(owner * ROWS, ROWS), ROWS)]
        start = pl.multiple_of(owner * ROWS + half * (ROWS // 2), ROWS // 2)
        return pool.at[pl.ds(start, ROWS // 2)]

    pool[pl.ds(pl.multiple_of(seat * ROWS, ROWS), ROWS), :] = vis[...].astype(jnp.bfloat16)
    pl.semaphore_wait(barrier, len(planes) + len(mates))

    for t in mates:
        remote(
            own_tickets, line_tickets.at[pl.ds(desk, 1)], tick_sems.at[0], tick_sems.at[1], t
        ).start()
    sends = []

    def pass_on(owner, half, send, recv, t):
        copy = remote(block(owner, half), block(owner, half), send, recv, t)
        copy.start()
        sends.append(copy)

    opposite = lax.rem(seat + 2, GROUP)
    pass_on(seat, 0, ring_send.at[0], ring_recv.at[0], partner)
    pass_on(seat, 1, ring_send.at[1], ring_recv.at[1], partner)
    pass_on(seat, None, pair_send.at[0], pair_recv, sibling)

    wait_bytes(line_tickets.at[pl.ds(0, LINE - 1)], tick_sems.at[1])
    my_rows = pl.ds(pl.multiple_of(front, LINE), LINE)
    all_tickets[my_rows, :] = line_tickets[...]
    for t in planes:
        remote(
            line_tickets, all_tickets.at[my_rows], tick_sems.at[2], tick_sems.at[3], t
        ).start()

    lower = lax.broadcasted_iota(jnp.int32, (ROWS, ROWS), 0) <= lax.broadcasted_iota(
        jnp.int32, (ROWS, ROWS), 1
    )
    mine = line_tickets[pl.ds(pl.multiple_of(desk - seat, GROUP), GROUP), :]
    inner = jnp.dot(
        mine.astype(jnp.float32).astype(jnp.bfloat16),
        jnp.where(lower, 1.0, 0.0).astype(jnp.bfloat16),
        preferred_element_type=jnp.float32,
    )
    loads[6].wait()
    wait_bytes(all_tickets.at[pl.ds(0, ROWS - LINE)], tick_sems.at[3])
    device = lax.broadcasted_iota(jnp.int32, (ROWS, 1), 0)
    lane = lax.broadcasted_iota(jnp.int32, (1, ROWS), 1)
    everything = all_tickets[...].astype(jnp.float32)
    totals = jnp.sum(everything, axis=1, keepdims=True)
    grand = jnp.sum(totals, axis=0, keepdims=True).astype(jnp.int32)
    z_high, z_low = grand >> SHIFT, grand & (CHAINS - 1)
    jitter = offset_ref[...]

    lines = jnp.sum(
        jnp.where(device // GROUP == lane // GROUP, totals, 0.0), axis=0, keepdims=True
    )
    most = jnp.max(lines, axis=1, keepdims=True).astype(jnp.int32)
    spill_ref[0, 0] = jnp.where(most * ROWS <= cap * grand, 0, 1)[0, 0]

    def point(k):
        return k * z_high + ((k * z_low + jitter) >> SHIFT)

    def count(mask, axis):
        return jnp.sum(jnp.where(mask, 1.0, 0.0), axis=axis, keepdims=True).astype(jnp.int32)

    before = jnp.sum(jnp.where(device < base, totals, 0.0), axis=0, keepdims=True)
    group_first = before.astype(jnp.int32)

    slot_row = lax.broadcasted_iota(jnp.int32, (GROUPS * cap, 1), 0)
    turn = slot_row // cap
    spot = 4 * ((gx + turn // 8) & 3) + ((gz + turn // 2) & 3)
    heir = 8 * spot + 2 * (line + (turn & 1) * (3 - 2 * line)) + core
    first = count(point(lane * ROWS + heir) < group_first, 1)
    place = first + (slot_row & (cap - 1))
    level = jnp.where(place < ROWS, point(place * ROWS + heir), jnp.int32(1 << 30))
    opened = before
    for d in range(GROUP):
        high = (opened + inner[d : d + 1, :]).astype(jnp.int32)
        low = high - mine[d : d + 1, :]
        onehot[:, d * ROWS : (d + 1) * ROWS] = jnp.where(
            (level >= low) & (level < high), 1.0, 0.0
        ).astype(jnp.bfloat16)
        opened = opened + inner[d : d + 1, ROWS - 1 : ROWS]

    for half in range(2):
        wait_bytes(block(opposite, half), ring_recv.at[half])
        pass_on(opposite, half, pair_send.at[1 + half], pair_recv, sibling)
    wait_bytes(pool.at[pl.ds(0, 2 * ROWS)], pair_recv)

    def ship(i):
        remote(
            outbox.at[pl.ds(i, 1)], inbox.at[pl.ds(group, 1)], rows_send, rows_recv, away(i)
        ).start()

    share = ROWS // cap
    for part in range(0, GROUPS, share):
        chunk = slice(part * cap, part * cap + ROWS)
        picked = jnp.dot(onehot[chunk, :], pool[...], preferred_element_type=jnp.float32)
        outbox[part : part + share] = picked.reshape(share, cap, 1024).astype(jnp.bfloat16)
    inbox[pl.ds(group, 1)] = outbox[0:1]
    for i in order:
        ship(i)

    loads[2].wait()

    def turn_over(i, carry):
        cols = pl.ds(pl.multiple_of(i * 256, 256), 256)
        for j in range(0, 1024, 256):
            cpl_t[cols, j : j + 256] = cpl[j : j + 256, cols].T
        return carry

    lax.fori_loop(0, 8, turn_over, 0)

    mark = lax.broadcasted_iota(jnp.int32, (1, GROUPS * cap), 1)
    origin = mark // cap
    opens = jnp.sum(
        jnp.where(device < GROUP * origin, totals, 0.0), axis=0, keepdims=True
    ).astype(jnp.int32)
    closes = jnp.sum(
        jnp.where(device < GROUP * origin + GROUP, totals, 0.0), axis=0, keepdims=True
    ).astype(jnp.int32)
    needs = point(device * ROWS + me)
    skipped = count(needs < opens, 0)
    chosen = (device - skipped == (mark & (cap - 1))) & (needs >= opens) & (needs < closes)
    selector = jnp.where(chosen, 1.0, 0.0).astype(jnp.bfloat16)

    for copy in loads[3:6]:
        copy.wait()
    wait_bytes(inbox.at[pl.ds(0, GROUPS - 1)], rows_recv)
    arrived = inbox[...].astype(jnp.float32).reshape(GROUPS * cap, 1024).astype(jnp.bfloat16)
    start = jnp.dot(selector, arrived, preferred_element_type=jnp.float32)
    vis[...] = start
    visb[...] = start.astype(jnp.bfloat16)

    def sweep(s, carry):
        for n in range(0, 2048, 256):
            cols = slice(n, n + 256)
            pre = jnp.dot(visb[...], cpl[:, cols], preferred_element_type=jnp.float32)
            field = pre + hb[:, cols] + nz[s, :, cols].astype(jnp.float32)
            hid[:, cols] = logistic(field).astype(jnp.bfloat16)
        for n in range(0, 1024, 256):
            cols = slice(n, n + 256)
            pre = jnp.dot(hid[...], cpl_t[:, cols], preferred_element_type=jnp.float32)
            new = 0.5 * vis[:, cols] + 0.5 * logistic(pre + vb[:, cols])
            vis[:, cols] = new
            visb[:, cols] = new.astype(jnp.bfloat16)
        return carry

    if cap == NARROW:
        for s in range(SWEEPS):
            sweep(s, 0)
    else:
        lax.fori_loop(0, SWEEPS, sweep, 0)
    result = pltpu.make_async_copy(vis, visible_ref, out_sem)
    result.start()

    energy = jnp.sum(vis[...] * vb[...], axis=1, keepdims=True)
    for n in range(0, 2048, 256):
        cols = slice(n, n + 256)
        act = jnp.dot(visb[...], cpl[:, cols], preferred_element_type=jnp.float32) + hb[:, cols]
        soft = jnp.maximum(act, 0.0) + jnp.log(1.0 + jnp.exp(-jnp.abs(act)))
        energy = energy + jnp.sum(soft, axis=1, keepdims=True)
    beta_step = 204.8 / 2048
    log_weight = beta_step * energy
    diagonal = device == lane
    flat = jnp.sum(jnp.where(diagonal, log_weight, 0.0), axis=0, keepdims=True)

    def packed(top, total):
        return jnp.where(lane < ROWS // 2, top, total)

    def merged(ref):
        both = ref[...]
        sums = pltpu.roll(both, ROWS // 2, 1)
        head = lax.broadcasted_iota(jnp.int32, both.shape, 1) < ROWS // 2
        top = jnp.max(jnp.where(head, both, -jnp.inf), axis=(0, 1), keepdims=True)
        one = lax.broadcasted_iota(jnp.int32, both.shape, 1) == 0
        scaled = jnp.where(one, sums * jnp.exp(jnp.where(one, both, top) - top), 0.0)
        return top, jnp.sum(scaled, axis=(0, 1), keepdims=True)

    top = jnp.max(flat, axis=1, keepdims=True)
    total = jnp.sum(jnp.exp(flat - top), axis=1, keepdims=True)
    own_stat[...] = packed(top, total)
    all_stats[pl.ds(me, 1), :] = packed(top, total)
    for t in everyone():
        pltpu.make_async_remote_copy(
            src_ref=own_stat,
            dst_ref=all_stats.at[pl.ds(me, 1)],
            send_sem=stat_sems.at[0],
            recv_sem=stat_sems.at[1],
            device_id=t,
            device_id_type=MESH,
        ).start()

    for copy in sends:
        copy.wait_send()
    wait_bytes(line_tickets.at[pl.ds(0, LINE - 1)], tick_sems.at[0])
    wait_bytes(all_tickets.at[pl.ds(0, ROWS - LINE)], tick_sems.at[2])
    wait_bytes(outbox.at[pl.ds(1, GROUPS - 1)], rows_send)

    wait_bytes(all_stats.at[pl.ds(0, ROWS - 1)], stat_sems.at[1])
    top, total = merged(all_stats)
    small_ref[:, :ROWS] = jnp.exp(flat - top) * (CHAINS / total)
    ratio = top + jnp.log(total) - jnp.log(jnp.full((1, 1), CHAINS, jnp.float32))
    small_ref[:, ROWS:] = jnp.broadcast_to(ratio, (1, ROWS))
    wait_bytes(all_stats.at[pl.ds(0, ROWS - 1)], stat_sems.at[0])
    result.wait()


def finish_kernel(visible, small, visible_out, weights_out, ratio_out, ratio, sems):
    ratio[...] = small[:, ROWS : ROWS + 1]
    copies = [
        pltpu.make_async_copy(src, dst, sems.at[i])
        for i, (src, dst) in enumerate(
            ((visible, visible_out), (small.at[:, pl.ds(0, ROWS)], weights_out), (ratio, ratio_out))
        )
    ]
    for copy in copies:
        copy.start()
    for copy in copies:
        copy.wait()


def run(cap, ident, *arrays):
    f32, b16, i32 = jnp.float32, jnp.bfloat16, jnp.int32
    anywhere = pl.BlockSpec(memory_space=pl.ANY)
    dma = pltpu.SemaphoreType.DMA
    return pl.pallas_call(
        functools.partial(step_kernel, cap),
        out_shape=(
            jax.ShapeDtypeStruct((ROWS, 1024), f32),
            jax.ShapeDtypeStruct((1, 2 * ROWS), f32),
            jax.ShapeDtypeStruct((1, 1), i32),
        ),
        in_specs=[anywhere] * 7,
        out_specs=(
            anywhere,
            pl.BlockSpec(memory_space=pltpu.VMEM),
            pl.BlockSpec(memory_space=pltpu.SMEM),
        ),
        scratch_shapes=[
            pltpu.VMEM((1, 1), i32),
            pltpu.VMEM((1, ROWS), i32),
            pltpu.VMEM((LINE, ROWS), i32),
            pltpu.VMEM((ROWS, ROWS), i32),
            pltpu.VMEM((ROWS, 1024), f32),
            pltpu.VMEM((GROUP * ROWS, 1024), b16),
            pltpu.VMEM((GROUPS * cap, GROUP * ROWS), b16),
            pltpu.VMEM((GROUPS, cap, 1024), b16),
            pltpu.VMEM((GROUPS, cap, 1024), b16),
            pltpu.VMEM((1024, 2048), b16),
            pltpu.VMEM((2048, 1024), b16),
            pltpu.VMEM((SWEEPS, ROWS, 2048), b16),
            pltpu.VMEM((1, 2048), f32),
            pltpu.VMEM((1, 1024), f32),
            pltpu.VMEM((ROWS, 2048), b16),
            pltpu.VMEM((ROWS, 1024), b16),
            pltpu.VMEM((1, ROWS), f32),
            pltpu.VMEM((ROWS, ROWS), f32),
            dma((7,)),
            dma((4,)),
            dma((2,)),
            dma((2,)),
            dma((3,)),
            dma(()),
            dma(()),
            dma(()),
            dma((2,)),
            dma(()),
        ],
        compiler_params=pltpu.CompilerParams(collective_id=ident, has_side_effects=True),
    )(*arrays)


def per_device(states, coupling, vis_bias, hid_bias, noise, tickets, offset):
    arrays = (
        states,
        coupling,
        vis_bias.reshape(1, 1024),
        hid_bias.reshape(1, 2048),
        noise,
        tickets.reshape(1, ROWS),
        offset.reshape(1, 1),
    )
    visible, small, spill = run(NARROW, 1, *arrays)
    visible, small = lax.cond(
        spill[0, 0] > 0,
        lambda kept: tuple(run(WIDE, 2, *arrays)[:2]),
        lambda kept: kept,
        (visible, small),
    )
    inside = pl.BlockSpec(memory_space=pltpu.VMEM)
    outside = pl.BlockSpec(memory_space=pl.ANY)
    visible, weights, ratio = pl.pallas_call(
        finish_kernel,
        out_shape=tuple(
            jax.ShapeDtypeStruct(shape, jnp.float32) for shape in ((ROWS, 1024), (1, ROWS), (1, 1))
        ),
        in_specs=[inside] * 2,
        out_specs=[outside] * 3,
        scratch_shapes=[pltpu.VMEM((1, 1), jnp.float32), pltpu.SemaphoreType.DMA((3,))],
    )(visible, small)
    return visible, weights.reshape(ROWS), ratio.reshape(())


def solution(mesh):
    both = ("grp", "rep")
    return jax.shard_map(
        per_device,
        mesh=mesh,
        in_specs=(P(both, None), P(), P(), P(), P(None, both, None), P(both), P()),
        out_specs=(P(both, None), P(both), P()),
        check_vma=False,
    )
```
